32 devices in a mesh: fsdp: 16 (over z, y, x), dp: 2 (over core).
Axes of the slice: x: 2, y: 2, z: 4, core: 2. Of those that a mesh axis runs over, the one named last changes fastest.
Arguments:
- gradients: bfloat16 [2, 64, 256, 256], P('dp', 'fsdp'), may hold values from -6 to 6
- first_moment: float32 [96, 256, 256], P('fsdp'), may hold values from -4 to 4
- second_moment: float32 [96, 256, 256], P('fsdp'), may hold values from 0.05 to 2
- left_basis: float32 [96, 256, 256], P('fsdp'), may hold values from -1 to 1, as said below
- right_basis: float32 [96, 256, 256], P('fsdp'), may hold values from -1 to 1, as said below
- shard_starts: int32 [16], replicated, may hold values from 0 to 48, as said below
- block_owners: int32 [48], replicated, may hold values from 0 to 15, as said below
Outputs:
- direction: float32 [64, 256, 256], P('fsdp')
- first_new: float32 [96, 256, 256], P('fsdp')
- second_new: float32 [96, 256, 256], P('fsdp')
The draws below stay inside these ranges and needn't reach their ends.
Inputs may be any that keep to these rules, and one draw needn't show every extreme that they name: Starts never fall and shard_starts[0] = 0; a device holds at most 4 blocks, some device exactly 4 and some none. `block_owners`: never falls; a device owns at most 6 blocks, some device exactly 6 and some none; a block's owner differs from its holder by at most 2 fsdp indices, by exactly 2 for some block in each direction. `left_basis`: each matrix is orthogonal up to float32 rounding. `right_basis`: each matrix is orthogonal up to float32 rounding.
All inputs are finite; a program needn't handle non-finite values.
Results may differ from the reference program's by a relative error of at most 0.0014.
Values may be sent and summed in bfloat16 or wider, within the bound.
A program may use at most 64 MiB of HBM per device.

```python
import math
import jax
import jax.numpy as jnp
import numpy as np
from jax import lax

BS = 256
SLOTS = 4
OWN = 6
STEP = 10
NBLK = 48
N_FSDP = 16
N_DP = 2


holder_table = np.array([[4, 4, 2, 2], [4, 3, 3, 2], [4, 4, 3, 1], [4, 4, 4, 0], [4, 3, 4, 1], [4, 2, 2, 4]], dtype=np.int32)


owner_table = np.array([[6, 2, 2, 2], [6, 3, 2, 1], [6, 4, 1, 1], [6, 6, 0, 0], [6, 3, 3, 0], [6, 4, 2, 0], [6, 5, 1, 0], [6, 1, 2, 3]], dtype=np.int32)


edge_holder_table = np.array([[4, 2], [3, 3], [2, 4]], dtype=np.int32)


edge_owner_table = np.array([[3, 3], [4, 2], [2, 4], [6, 0], [0, 6]], dtype=np.int32)


def group_counts(key):
    inner = N_FSDP // 4 - 1
    middle = N_FSDP // 8 - 1
    base = jax.random.fold_in(key, 7)
    parts = jax.random.split(base, 8)
    hold_pick = jax.random.randint(parts[0], (inner,), 0, holder_table.shape[0])
    own_pick = jax.random.randint(parts[1], (inner,), 0, owner_table.shape[0])
    hold_rows = jnp.asarray(holder_table)[hold_pick]
    own_rows = jnp.asarray(owner_table)[own_pick]
    hold_keys = jax.random.split(parts[2], inner)
    own_keys = jax.random.split(parts[3], inner)
    hold_rows = jax.vmap(lambda kk, row: jax.random.permutation(kk, row))(hold_keys, hold_rows)
    own_rows = jax.vmap(lambda kk, row: jax.random.permutation(kk, row))(own_keys, own_rows)
    first_rank = jax.random.randint(parts[4], (), 0, inner - 1)
    first_group = first_rank + (first_rank >= middle).astype(jnp.int32)
    second_rank = (first_rank + 1 + jax.random.randint(parts[5], (), 0, inner - 2)) % (inner - 1)
    second_group = second_rank + (second_rank >= middle).astype(jnp.int32)
    group_ids = jnp.arange(inner)[:, None]
    hold_rows = jnp.where(group_ids == first_group, jnp.array([[4, 4, 4, 0]], jnp.int32), hold_rows)
    own_rows = jnp.where(group_ids == first_group, jnp.array([[0, 0, 6, 6]], jnp.int32), own_rows)
    hold_rows = jnp.where(group_ids == second_group, jnp.array([[0, 4, 4, 4]], jnp.int32), hold_rows)
    own_rows = jnp.where(group_ids == second_group, jnp.array([[6, 6, 0, 0]], jnp.int32), own_rows)
    hold_rows = jnp.where(group_ids == middle, jnp.array([[4, 4, 4, 0]], jnp.int32), hold_rows)
    own_rows = jnp.where(group_ids == middle, jnp.array([[0, 2, 6, 4]], jnp.int32), own_rows)
    edge_keys = jax.random.split(parts[6], 2)
    owner_keys = jax.random.split(parts[7], 2)
    edge_hold = [jnp.asarray(edge_holder_table)[jax.random.randint(edge_keys[side], (), 0, edge_holder_table.shape[0])] for side in range(2)]
    edge_own = [jnp.asarray(edge_owner_table)[jax.random.randint(owner_keys[side], (), 0, edge_owner_table.shape[0])] for side in range(2)]
    hold_counts = jnp.concatenate([edge_hold[0], hold_rows.reshape(-1), edge_hold[1]]).astype(jnp.int32)
    own_counts = jnp.concatenate([edge_own[0], own_rows.reshape(-1), edge_own[1]]).astype(jnp.int32)
    return (hold_counts, own_counts)


def draw_shard_starts(key, part):
    hold_counts, own_counts = group_counts(key)
    return (jnp.cumsum(hold_counts) - hold_counts).astype(jnp.int32)


def draw_block_owners(key, part):
    hold_counts, own_counts = group_counts(key)
    return jnp.repeat(jnp.arange(N_FSDP, dtype=jnp.int32), own_counts, total_repeat_length=NBLK).astype(jnp.int32)


def orthogonal(key, spread):
    random_part = jax.random.normal(key, (N_FSDP * OWN, BS, BS), jnp.float32) * (spread / BS ** 0.5)
    skew_part = random_part - jnp.swapaxes(random_part, 1, 2)
    identity = jnp.broadcast_to(jnp.eye(BS, dtype=jnp.float32), skew_part.shape)
    return jnp.linalg.solve(identity - skew_part, identity + skew_part)


def draw_left_basis(key, part):
    return orthogonal(jax.random.fold_in(key, 11), 0.8)


def draw_right_basis(key, part):
    return orthogonal(jax.random.fold_in(key, 13), 0.8)


def shard_levels(key, shape, cuts, smallest, high):
    def one(axis_at, blocks):
        heights = jax.random.uniform(jax.random.fold_in(jax.random.fold_in(key, 6), axis_at), (blocks,), jnp.float32, smallest / len(cuts), high / len(cuts))
        return jnp.repeat(jnp.exp(heights), shape[axis_at] // blocks).reshape((-1,) + (1,) * (len(shape) - axis_at - 1))

    level = one(*cuts[0])
    for cut in cuts[1:]:
        level = level * one(*cut)
    return level


def gaussian(own_key, dims, scale, reach, shards=(), kind=jnp.bfloat16):
    gain = shard_levels(own_key, dims, shards, -0.22, 0.18) if shards else 1.0
    result = jax.random.normal(own_key, dims, jnp.float32) * scale * gain
    return jnp.minimum(jnp.maximum(result, -reach), reach).astype(kind)


def setup_inputs(seed: int = 0) -> dict:
    streams_of = jax.random.split(jax.random.key(seed), 8)
    return {
        "gradients": gaussian(streams_of[0], (N_DP, N_FSDP * SLOTS, BS, BS), 1.0, 6.0, ((0, 2), (1, 16))),
        "first_moment": gaussian(streams_of[1], (N_FSDP * OWN, BS, BS), 0.5, 4.0, ((0, 16),), jnp.float32),
        "second_moment": jnp.clip(jnp.exp(math.log(2.0) - 3.6888794 * jax.random.uniform(streams_of[2], (N_FSDP * OWN, BS, BS), jnp.float32) ** shard_levels(streams_of[2], (N_FSDP * OWN, BS, BS), ((0, 16),), -0.2, 0.2)), 0.05, 2.0),
        "left_basis": draw_left_basis(jax.random.fold_in(streams_of[7], 71), 0),
        "right_basis": draw_right_basis(jax.random.fold_in(streams_of[7], 71), 0),
        "shard_starts": draw_shard_starts(jax.random.fold_in(streams_of[7], 71), 0),
        "block_owners": draw_block_owners(jax.random.fold_in(streams_of[7], 71), 0),
    }


beta_one = 0.9
beta_two = 0.95
epsilon = 1e-08

def soap_blocks(gradient, moment_one, moment_two, left_basis, right_basis):
    highest = lax.Precision.HIGHEST
    moment_new = beta_one * moment_one + (1.0 - beta_one) * gradient
    turned = jnp.einsum('jad,jde->jae', jnp.einsum('jba,jbd->jad', left_basis, gradient, precision=highest), right_basis, precision=highest)
    turned_moment = jnp.einsum('jad,jde->jae', jnp.einsum('jba,jbd->jad', left_basis, moment_new, precision=highest), right_basis, precision=highest)
    second_next = beta_two * moment_two + (1.0 - beta_two) * turned * turned
    bias_one = 1.0 - beta_one ** STEP
    bias_two = 1.0 - beta_two ** STEP
    scaled = turned_moment / bias_one / (jnp.sqrt(second_next / bias_two) + epsilon)
    update = jnp.einsum('jad,jed->jae', jnp.einsum('jab,jbd->jad', left_basis, scaled, precision=highest), right_basis, precision=highest)
    return (moment_new, second_next, update)

def reference(gradients, first_moment, second_moment, left_basis, right_basis, shard_starts, block_owners):
    block_ids = jnp.arange(NBLK, dtype=jnp.int32)
    holder = (jnp.searchsorted(shard_starts, block_ids, side='right') - 1).astype(jnp.int32)
    hold_row = (holder * SLOTS + block_ids - shard_starts[holder]).astype(jnp.int32)
    first_owned = jnp.searchsorted(block_owners, block_owners, side='left').astype(jnp.int32)
    own_row = (block_owners * OWN + block_ids - first_owned).astype(jnp.int32)
    summed = lax.optimization_barrier(jnp.sum(gradients.astype(jnp.float32), axis=0)).astype(jnp.bfloat16)
    gradient = summed[hold_row].astype(jnp.float32)
    moment_new, second_next, update = soap_blocks(gradient, first_moment[own_row], second_moment[own_row], left_basis[own_row], right_basis[own_row])
    blank_hold = jnp.zeros((N_FSDP * SLOTS, BS, BS), jnp.float32)
    blank_own = jnp.zeros((N_FSDP * OWN, BS, BS), jnp.float32)
    direction = blank_hold.at[hold_row].set(update)
    first_new = blank_own.at[own_row].set(moment_new)
    second_new = blank_own.at[own_row].set(second_next)
    return (direction, first_new, second_new)
```

```python
import functools

import jax
import jax.numpy as jnp
from jax import lax
from jax.experimental import pallas as pl
from jax.experimental.pallas import tpu as pltpu
from jax.sharding import PartitionSpec as P

REACH = 2
SIDES = 2 * REACH + 1
STEP = 10
LEVELS = 32767.0

beta_one = 0.9
beta_two = 0.95
epsilon = 1e-08

MESH = pl.DeviceIdType.MESH


def ring_barrier(me, devices, core):
    barrier = pltpu.get_barrier_semaphore()
    pl.semaphore_signal(barrier, inc=1, device_id={"dp": 1 - core}, device_id_type=MESH)
    for side in range(SIDES):
        if side == REACH:
            continue
        other = me + side - REACH

        @pl.when((other >= 0) & (other < devices))
        def _():
            pl.semaphore_signal(barrier, inc=1, device_id={"fsdp": other}, device_id_type=MESH)

    below = jnp.minimum(me, REACH)
    above = jnp.minimum(devices - 1 - me, REACH)
    pl.semaphore_wait(barrier, 1 + below + above)


def in_range(me, side, devices):
    other = me + side - REACH
    return (other >= 0) & (other < devices)


def gather_kernel(devices, slots, g_ref, out_ref, part, rs_send, rs_recv, send, recv, fsend, frecv):
    me = lax.axis_index("fsdp")
    core = lax.axis_index("dp")
    half = g_ref.shape[2] // 2
    mine = pl.ds(pl.multiple_of(core * half, half), half)
    theirs = pl.ds(pl.multiple_of((1 - core) * half, half), half)
    partner = {"dp": 1 - core}

    def reduce_copy(s):
        return pltpu.make_async_remote_copy(
            g_ref.at[0, s, theirs], part.at[s], rs_send.at[s], rs_recv.at[s], partner, MESH
        )

    def send_copy(side, s):
        return pltpu.make_async_remote_copy(
            out_ref.at[REACH * slots + s, mine],
            out_ref.at[(SIDES - 1 - side) * slots + s, mine],
            send.at[side * slots + s],
            recv.at[(SIDES - 1 - side) * slots + s],
            {"fsdp": me + side - REACH},
            MESH,
        )

    def arrival(side, s):
        at = side * slots + s
        return pltpu.make_async_remote_copy(
            out_ref.at[at, mine], out_ref.at[at, mine], send.at[at], recv.at[at], partner, MESH
        )

    def forward(side, s, rows):
        at = side * slots + s
        return pltpu.make_async_remote_copy(
            out_ref.at[at, rows], out_ref.at[at, rows], fsend.at[at], frecv.at[at], partner, MESH
        )

    ring_barrier(me, devices, core)
    for s in range(slots):
        reduce_copy(s).start()
    for s in range(slots):
        reduce_copy(s).wait_recv()
        total = g_ref[0, s, mine].astype(jnp.float32) + part[s].astype(jnp.float32)
        out_ref[REACH * slots + s, mine] = total.astype(jnp.bfloat16)
        for side in (0, 4, 1, 3):

            @pl.when(in_range(me, side, devices))
            def _():
                send_copy(side, s).start()

        forward(REACH, s, mine).start()
    for s in range(slots):
        for side in (0, 4, 1, 3):

            @pl.when(in_range(me, side, devices))
            def _():
                arrival(side, s).wait_recv()
                forward(side, s, mine).start()

    for s in range(slots):
        reduce_copy(s).wait_send()
        forward(REACH, s, mine).wait_send()
        forward(REACH, s, theirs).wait_recv()
        for side in (0, 4, 1, 3):

            @pl.when(in_range(me, side, devices))
            def _():
                send_copy(side, s).wait_send()
                forward(side, s, mine).wait_send()
                forward(side, s, theirs).wait_recv()


def return_kernel(
    devices, slots, q_ref, w_ref, out_ref, wout_ref,
    lsem, send, recv, fsend, frecv, wl, wsend, wrecv, wfsend, wfrecv,
):
    me = lax.axis_index("fsdp")
    core = lax.axis_index("dp")
    half = q_ref.shape[1]
    mine = pl.ds(pl.multiple_of(core * half, half), half)
    theirs = pl.ds(pl.multiple_of((1 - core) * half, half), half)
    partner = {"dp": 1 - core}

    def group(side):
        return pl.ds(side * slots, slots)

    def send_copy(side, s):
        return pltpu.make_async_remote_copy(
            q_ref.at[side * slots + s],
            out_ref.at[(SIDES - 1 - side) * slots + s, mine],
            send.at[side * slots + s],
            recv.at[(SIDES - 1 - side) * slots + s],
            {"fsdp": me + side - REACH},
            MESH,
        )

    def send_scale(side):
        return pltpu.make_async_remote_copy(
            w_ref.at[group(side)],
            wout_ref.at[core, group(SIDES - 1 - side)],
            wsend.at[side],
            wrecv.at[SIDES - 1 - side],
            {"fsdp": me + side - REACH},
            MESH,
        )

    def arrival(side, s):
        at = side * slots + s
        return pltpu.make_async_remote_copy(
            out_ref.at[at, mine], out_ref.at[at, mine], send.at[at], recv.at[at], partner, MESH
        )

    def arrival_scale(side):
        return pltpu.make_async_remote_copy(
            wout_ref.at[core, group(side)], wout_ref.at[core, group(side)],
            wsend.at[side], wrecv.at[side], partner, MESH,
        )

    def forward(side, s, rows):
        at = side * slots + s
        source = q_ref.at[at] if side == REACH else out_ref.at[at, rows]
        return pltpu.make_async_remote_copy(
            source, out_ref.at[at, rows], fsend.at[at], frecv.at[at], partner, MESH
        )

    def forward_scale(side, which):
        source = w_ref.at[group(side)] if side == REACH else wout_ref.at[which, group(side)]
        return pltpu.make_async_remote_copy(
            source, wout_ref.at[which, group(side)],
            wfsend.at[side], wfrecv.at[side], partner, MESH,
        )

    keep = [
        pltpu.make_async_copy(
            q_ref.at[REACH * slots + s], out_ref.at[REACH * slots + s, mine], lsem.at[s]
        )
        for s in range(slots)
    ]
    keep.append(
        pltpu.make_async_copy(w_ref.at[group(REACH)], wout_ref.at[core, group(REACH)], wl)
    )
    ring_barrier(me, devices, core)
    for side in (0, 4, 1, 3):

        @pl.when(in_range(me, side, devices))
        def _():
            send_scale(side).start()

    for s in range(slots):
        for side in (0, 4, 1, 3):

            @pl.when(in_range(me, side, devices))
            def _():
                send_copy(side, s).start()

    for s in range(slots):
        forward(REACH, s, mine).start()
    forward_scale(REACH, core).start()
    for copy in keep:
        copy.start()
    for side in (0, 4, 1, 3):

        @pl.when(in_range(me, side, devices))
        def _():
            arrival_scale(side).wait_recv()
            forward_scale(side, core).start()

    for s in range(slots):
        for side in (0, 4, 1, 3):

            @pl.when(in_range(me, side, devices))
            def _():
                arrival(side, s).wait_recv()
                forward(side, s, mine).start()

    for copy in keep:
        copy.wait()
    for side in range(SIDES):

        @pl.when(in_range(me, side, devices))
        def _():
            forward_scale(side, core).wait_send()
            forward_scale(side, 1 - core).wait_recv()
            if side != REACH:
                send_scale(side).wait_send()
            for s in range(slots):
                forward(side, s, mine).wait_send()
                forward(side, s, theirs).wait_recv()
                if side != REACH:
                    send_copy(side, s).wait_send()


def split(value):
    high = value.astype(jnp.bfloat16)
    low = (value - high.astype(jnp.float32)).astype(jnp.bfloat16)
    return high, low


def dot(a, b, dims=((1,), (0,))):
    return lax.dot_general(a, b, (dims, ((), ())), preferred_element_type=jnp.float32)


def step_kernel(place_ref, from_ref, live_ref, core_ref, g_ref, m_ref, v_ref, l_ref, r_ref,
                mo_ref, vo_ref, q_ref, w_ref):
    j = pl.program_id(0)
    half = q_ref.shape[1]
    width = g_ref.shape[2]
    live = live_ref[j] > 0

    @pl.when(live)
    def _():
        gradient = g_ref[0]
        moment = beta_one * m_ref[0] + (1.0 - beta_one) * gradient.astype(jnp.float32)
        mo_ref[0] = moment
        left_high, left_low = split(l_ref[0])
        right_high, right_low = split(r_ref[0])
        moment_high, moment_low = split(moment)
        first = ((0,), (0,))
        grad_side = dot(left_high, gradient, first) + dot(left_low, gradient, first)
        moment_side = (
            dot(left_high, moment_high, first)
            + dot(left_high, moment_low, first)
            + dot(left_low, moment_high, first)
        )
        both_high, both_low = split(jnp.concatenate([grad_side, moment_side], axis=0))
        turned = dot(both_high, right_high) + dot(both_high, right_low) + dot(both_low, right_high)
        turned_gradient = turned[:width]
        turned_moment = turned[width:]
        second = beta_two * v_ref[0] + (1.0 - beta_two) * turned_gradient * turned_gradient
        vo_ref[0] = second
        bias_one = 1.0 - beta_one**STEP
        bias_two = 1.0 - beta_two**STEP
        scaled = turned_moment / bias_one / (jnp.sqrt(second / bias_two) + epsilon)
        scaled_high, scaled_low = split(scaled)
        rows = pl.ds(pl.multiple_of(core_ref[0] * half, half), half)
        part_high, part_low = split(l_ref[0, rows])
        back = (
            dot(part_high, scaled_high) + dot(part_high, scaled_low) + dot(part_low, scaled_high)
        )
        back_high, back_low = split(back)
        last = ((1,), (1,))
        update = (
            dot(back_high, right_high, last)
            + dot(back_high, right_low, last)
            + dot(back_low, right_high, last)
        )
        peak = jnp.maximum(jnp.max(jnp.abs(update), axis=0, keepdims=True), 1e-30)
        q_ref[0] = jnp.round(update * (LEVELS / peak)).astype(jnp.int32).astype(jnp.int16)
        w_ref[0] = peak * (1.0 / LEVELS)

    @pl.when(jnp.logical_not(live))
    def _():
        mo_ref[...] = jnp.zeros_like(mo_ref)
        vo_ref[...] = jnp.zeros_like(vo_ref)
        q_ref[...] = jnp.zeros_like(q_ref)
        w_ref[...] = jnp.zeros_like(w_ref)


def place_kernel(from_ref, live_ref, q_ref, w_ref, d_ref):
    s = pl.program_id(0)
    half = q_ref.shape[1] // 2
    live = live_ref[s] > 0

    @pl.when(live)
    def _():
        for c in range(2):
            rows = pl.ds(c * half, half)
            d_ref[0, rows] = q_ref[0, rows].astype(jnp.int32).astype(jnp.float32) * w_ref[c, 0]

    @pl.when(jnp.logical_not(live))
    def _():
        d_ref[...] = jnp.zeros_like(d_ref)


def body(
    gradients, first_moment, second_moment, left_basis, right_basis, shard_starts, block_owners
):
    devices = lax.axis_size("fsdp")
    me = lax.axis_index("fsdp")
    core = lax.axis_index("dp")
    slots = gradients.shape[1]
    owned = first_moment.shape[0]
    width = gradients.shape[3]
    half = width // lax.axis_size("dp")
    blocks = block_owners.shape[0]
    places = SIDES * slots

    own_first = jnp.sum((block_owners < me).astype(jnp.int32))
    own_count = jnp.sum((block_owners == me).astype(jnp.int32))
    own_block = own_first + jnp.arange(owned, dtype=jnp.int32)
    passed = shard_starts[None, :] <= own_block[:, None]
    holder = jnp.sum(passed.astype(jnp.int32), axis=1) - 1
    holder_start = jnp.max(jnp.where(passed, shard_starts[None, :], 0), axis=1)
    own_live = (jnp.arange(owned) < own_count).astype(jnp.int32)
    spot = (holder - me + REACH) * slots + own_block - holder_start
    own_place = jnp.where(own_live > 0, spot, places)
    own_from = jnp.where(own_live > 0, spot, 0)

    starts = jnp.concatenate([shard_starts, jnp.full((1,), blocks, jnp.int32)])
    ids = jnp.arange(devices + 1)
    my_start = jnp.sum(jnp.where(ids == me, starts, 0))
    my_end = jnp.sum(jnp.where(ids == me + 1, starts, 0))
    slot_ids = jnp.arange(slots, dtype=jnp.int32)
    held_block = my_start + slot_ids
    held_live = (held_block < my_end).astype(jnp.int32)
    held_owner = jnp.sum(
        jnp.where(jnp.arange(blocks)[None, :] == held_block[:, None], block_owners[None, :], 0), axis=1
    )
    held_from = jnp.where(held_live > 0, (held_owner - me + REACH) * slots + slot_ids, 0)

    vmem = pl.BlockSpec(memory_space=pltpu.VMEM)
    dma = pltpu.SemaphoreType.DMA
    gathered = pl.pallas_call(
        functools.partial(gather_kernel, devices, slots),
        out_shape=jax.ShapeDtypeStruct((places, width, width), jnp.bfloat16),
        in_specs=[vmem],
        out_specs=vmem,
        scratch_shapes=[
            pltpu.VMEM((slots, half, width), jnp.bfloat16),
            dma((slots,)),
            dma((slots,)),
            dma((places,)),
            dma((places,)),
            dma((places,)),
            dma((places,)),
        ],
        compiler_params=pltpu.CompilerParams(collective_id=0, has_side_effects=True),
        name="gather",
    )(gradients)

    def by_own(j, place, origin, live, core):
        return (j, 0, 0)

    square = (1, width, width)
    moment_new, second_next, packed, scales = pl.pallas_call(
        step_kernel,
        grid_spec=pltpu.PrefetchScalarGridSpec(
            num_scalar_prefetch=4,
            grid=(owned,),
            in_specs=[
                pl.BlockSpec(square, lambda j, place, origin, live, core: (origin[j], 0, 0)),
                pl.BlockSpec(square, by_own),
                pl.BlockSpec(square, by_own),
                pl.BlockSpec(square, by_own),
                pl.BlockSpec(square, by_own),
            ],
            out_specs=[
                pl.BlockSpec(square, by_own),
                pl.BlockSpec(square, by_own),
                pl.BlockSpec((1, half, width), lambda j, place, origin, live, core: (place[j], 0, 0)),
                pl.BlockSpec((1, 1, width), lambda j, place, origin, live, core: (place[j], 0, 0)),
            ],
        ),
        out_shape=[
            jax.ShapeDtypeStruct(first_moment.shape, jnp.float32),
            jax.ShapeDtypeStruct(first_moment.shape, jnp.float32),
            jax.ShapeDtypeStruct((places + 1, half, width), jnp.int16),
            jax.ShapeDtypeStruct((places + 1, 1, width), jnp.float32),
        ],
        name="step",
    )(own_place, own_from, own_live, core[None].astype(jnp.int32),
      gathered, first_moment, second_moment, left_basis, right_basis)

    returned, return_scales = pl.pallas_call(
        functools.partial(return_kernel, devices, slots),
        out_shape=[
            jax.ShapeDtypeStruct((places, width, width), jnp.int16),
            jax.ShapeDtypeStruct((2, places, 1, width), jnp.float32),
        ],
        in_specs=[vmem, vmem],
        out_specs=[vmem, vmem],
        scratch_shapes=[
            dma((slots,)),
            dma((places,)),
            dma((places,)),
            dma((places,)),
            dma((places,)),
            dma,
            dma((SIDES,)),
            dma((SIDES,)),
            dma((SIDES,)),
            dma((SIDES,)),
        ],
        compiler_params=pltpu.CompilerParams(collective_id=1, has_side_effects=True),
        name="give_back",
    )(packed, scales)

    direction = pl.pallas_call(
        place_kernel,
        grid_spec=pltpu.PrefetchScalarGridSpec(
            num_scalar_prefetch=2,
            grid=(slots,),
            in_specs=[
                pl.BlockSpec(square, lambda s, origin, live: (origin[s], 0, 0)),
                pl.BlockSpec((2, 1, 1, width), lambda s, origin, live: (0, origin[s], 0, 0)),
            ],
            out_specs=pl.BlockSpec(square, lambda s, origin, live: (s, 0, 0)),
        ),
        out_shape=jax.ShapeDtypeStruct((slots, width, width), jnp.float32),
        name="place",
    )(held_from, held_live, returned, return_scales)
    return (direction, moment_new, second_next)


def solution(mesh):
    in_specs = (
        P("dp", "fsdp", None, None),
        P("fsdp", None, None),
        P("fsdp", None, None),
        P("fsdp", None, None),
        P("fsdp", None, None),
        P(),
        P(),
    )
    out_specs = (P("fsdp", None, None), P("fsdp", None, None), P("fsdp", None, None))
    return jax.shard_map(body, mesh=mesh, in_specs=in_specs, out_specs=out_specs, check_vma=False)
```

```python
import functools

import jax
import jax.numpy as jnp
from jax import lax
from jax.experimental import pallas as pl
from jax.experimental.pallas import tpu as pltpu
from jax.sharding import PartitionSpec as P

REACH = 2
SIDES = 2 * REACH + 1
STEP = 10
LEVELS = 32767.0

beta_one = 0.9
beta_two = 0.95
epsilon = 1e-08

MESH = pl.DeviceIdType.MESH


DIRECT = ((1, 2), (-1, 2), (1, -2), (-1, -2))

ONWARD = (
    ({1: (2,), 2: (4,)}, {2: (4,), -2: (-1,)}, {-2: (-4,), 2: (1,)}, {-2: (-4,), -1: (-2,)}),
    (
        {2: (4, 1)},
        {-1: (-4,), 3: (2,), 2: (4,)},
        {-2: (-4,), 1: (4,), -3: (-2,)},
        {-2: (-1, -4)},
    ),
)

HOPS = (
    {1: 1, 2: 1, -2: 2, -1: 3},
    {-1: 1, 2: 1, 1: 2, -2: 2, 3: 2},
    {-2: 1, 1: 1, -1: 2, 2: 2, -3: 2},
    {-1: 1, -2: 1, 2: 2, 1: 3},
)


def guarded(condition, action):
    if condition is None:
        action()
    else:
        pl.when(condition)(action)


def greet(me, core, devices):
    barrier = pltpu.get_barrier_semaphore()
    x = jnp.where(me % 2 == 0, me + 1, me - 1)
    y = jnp.where(me % 4 < 2, me + 2, me - 2)
    pl.semaphore_signal(barrier, inc=1, device_id={"dp": 1 - core}, device_id_type=MESH)
    pl.semaphore_signal(barrier, inc=1, device_id={"fsdp": x}, device_id_type=MESH)
    pl.semaphore_signal(barrier, inc=1, device_id={"fsdp": y}, device_id_type=MESH)

    @pl.when(me >= 4)
    def _():
        pl.semaphore_signal(barrier, inc=1, device_id={"fsdp": me - 4}, device_id_type=MESH)

    @pl.when(me + 4 < devices)
    def _():
        pl.semaphore_signal(barrier, inc=1, device_id={"fsdp": me + 4}, device_id_type=MESH)

    return barrier


def met(barrier, me, devices):
    outer = jnp.where(me >= 4, 1, 0) + jnp.where(me + 4 < devices, 1, 0)
    pl.semaphore_wait(barrier, 3 + outer)


def relay(me, place, core, devices, items, own, ready, land, osend, fsend, recv, dsend, drecv):
    partner = {"dp": 1 - core}
    below, above = me >= 4, me + 4 < devices

    def reach(step):
        to = place + step
        return below if to < 0 else above if to > 3 else None

    def own_copy(way, i):
        hop = DIRECT[place][way]
        return pltpu.make_async_remote_copy(
            own(i), land(-hop, i, core), osend.at[way * items + i],
            recv.at[(3 - hop) * items + i], {"fsdp": me + hop}, MESH,
        )

    routes = [(off, hop) for off, hops in ONWARD[core][place].items() for hop in hops]

    def onward(off, hop, i):
        return pltpu.make_async_remote_copy(
            land(off, i, core), land(off - hop, i, core),
            fsend.at[routes.index((off, hop)) * items + i],
            recv.at[(off - hop + 3) * items + i], {"fsdp": me + hop}, MESH,
        )

    def arrival(off, i):
        at = recv.at[(off + 3) * items + i]
        ref = land(off, i, core)
        return pltpu.make_async_remote_copy(ref, ref, at, at, partner, MESH)

    def across(off, i, which):
        at = (off + REACH) * items + i
        source = own(i) if off == 0 else land(off, i, which)
        return pltpu.make_async_remote_copy(
            source, land(off, i, which), dsend.at[at], drecv.at[at], partner, MESH
        )

    offsets = [off for off in HOPS[place] if abs(off) <= REACH or off in ONWARD[core][place]]
    for i in range(items):
        ready(i)
        for way in range(2):
            own_copy(way, i).start()
        across(0, i, core).start()
    order = sorted((i + 2 * (HOPS[place][off] - 1), off, i) for off in offsets for i in range(items))
    for _, off, i in order:

        def arrive(off=off, i=i):
            arrival(off, i).wait_recv()
            for hop in ONWARD[core][place].get(off, ()):
                guarded(reach(hop), lambda hop=hop: onward(off, hop, i).start())
            if abs(off) <= REACH:
                across(off, i, core).start()

        guarded(reach(off), arrive)
    for i in range(items):
        for way in range(2):
            own_copy(way, i).wait_send()
        across(0, i, core).wait_send()
        across(0, i, 1 - core).wait_recv()
    for off in offsets:

        def finish(off=off):
            for i in range(items):
                for hop in ONWARD[core][place].get(off, ()):
                    guarded(reach(hop), lambda hop=hop, i=i: onward(off, hop, i).wait_send())
                if abs(off) <= REACH:
                    across(off, i, core).wait_send()
                    across(off, i, 1 - core).wait_recv()

        guarded(reach(off), finish)


def tables(me, devices, slots, owned, starts_ref, owners_ref, table_ref):
    blocks = owners_ref.shape[0]
    start = starts_ref[me]
    end = jnp.where(me + 1 < devices, starts_ref[jnp.minimum(me + 1, devices - 1)], blocks)
    held_owner = [owners_ref[jnp.minimum(start + s, blocks - 1)] for s in range(slots)]

    def count(b, carry):
        owner = owners_ref[b]
        below, mine, *ahead = carry
        return (
            below + (owner < me).astype(jnp.int32),
            mine + (owner == me).astype(jnp.int32),
            *[n + (owner < held_owner[s]).astype(jnp.int32) for s, n in enumerate(ahead)],
        )

    zero = jnp.int32(0)
    first, mine, *ahead = lax.fori_loop(0, blocks, count, (zero,) * (2 + slots))

    def seek(i, carry):
        begin = starts_ref[i]
        found = []
        for j in range(owned):
            holder, at = carry[j]
            passed = begin <= first + j
            found.append(
                (jnp.where(passed, i, holder), jnp.where(passed, begin, at))
            )
        return tuple(found)

    found = lax.fori_loop(0, devices, seek, ((zero, zero),) * owned)
    for j in range(owned):
        holder, at = found[j]
        live = j < mine
        table_ref[j] = jnp.where(live, (holder - me + REACH) * slots + first + j - at, 0)
        table_ref[owned + j] = live.astype(jnp.int32)
    for s in range(slots):
        live = start + s < end
        spot = (held_owner[s] - me + REACH) * owned + start + s - ahead[s]
        table_ref[2 * owned + s] = jnp.where(live, spot, 0)
        table_ref[2 * owned + slots + s] = live.astype(jnp.int32)


def each_place(me, core, run):
    for place in range(4):
        for side in range(2):

            @pl.when((me % 4 == place) & (core == side))
            def _():
                run(place, side)


def gather_kernel(
    devices, slots, owned, starts_ref, owners_ref, g_ref, out_ref, table_ref,
    part, transit, rs_send, rs_recv, osend, fsend, recv, dsend, drecv,
):
    me = lax.axis_index("fsdp")
    core = lax.axis_index("dp")
    half = g_ref.shape[2] // 2
    barrier = greet(me, core, devices)
    tables(me, devices, slots, owned, starts_ref, owners_ref, table_ref)
    met(barrier, me, devices)

    def run(place, side):
        mine, theirs = pl.ds(side * half, half), pl.ds((1 - side) * half, half)

        def reduce_copy(s):
            return pltpu.make_async_remote_copy(
                g_ref.at[0, s, theirs], part.at[s], rs_send.at[s], rs_recv.at[s],
                {"dp": 1 - side}, MESH,
            )

        def ready(s):
            reduce_copy(s).wait_recv()
            total = g_ref[0, s, mine].astype(jnp.float32) + part[s].astype(jnp.float32)
            out_ref[REACH * slots + s, mine] = total.astype(jnp.bfloat16)

        def land(off, s, which):
            if abs(off) > REACH:
                return transit.at[s]
            return out_ref.at[(off + REACH) * slots + s, pl.ds(which * half, half)]

        for s in range(slots):
            reduce_copy(s).start()
        relay(me, place, side, devices, slots, lambda s: land(0, s, side), ready, land,
              osend, fsend, recv, dsend, drecv)
        for s in range(slots):
            reduce_copy(s).wait_send()

    each_place(me, core, run)


def return_kernel(
    devices, owned, q_ref, w_ref, out_ref, wout_ref,
    transit, wtransit, lsem, osend, fsend, recv, dsend, drecv,
):
    me = lax.axis_index("fsdp")
    core = lax.axis_index("dp")
    half = q_ref.shape[1]
    met(greet(me, core, devices), me, devices)

    def run(place, side):
        def own(i):
            return w_ref if i == 0 else q_ref.at[i - 1]

        def land(off, i, which):
            if i == 0:
                if abs(off) > REACH:
                    return wtransit
                return wout_ref.at[which, pl.ds((off + REACH) * owned, owned)]
            if abs(off) > REACH:
                return transit.at[i - 1]
            return out_ref.at[(off + REACH) * owned + i - 1, pl.ds(which * half, half)]

        def keep(i):
            return pltpu.make_async_copy(own(i), land(0, i, side), lsem.at[i])

        relay(me, place, side, devices, owned + 1, own, lambda i: keep(i).start(), land,
              osend, fsend, recv, dsend, drecv)
        for i in range(owned + 1):
            keep(i).wait()

    each_place(me, core, run)


def split(value):
    high = value.astype(jnp.bfloat16)
    low = (value - high.astype(jnp.float32)).astype(jnp.bfloat16)
    return high, low


def dot(a, b, dims=((1,), (0,))):
    return lax.dot_general(a, b, (dims, ((), ())), preferred_element_type=jnp.float32)


def step_kernel(table_ref, core_ref, g_ref, m_ref, v_ref, l_ref, r_ref,
                mo_ref, vo_ref, q_ref, w_ref):
    j = pl.program_id(0)
    half = q_ref.shape[1]
    width = g_ref.shape[2]
    live = table_ref[pl.num_programs(0) + j] > 0

    @pl.when(live)
    def _():
        gradient = g_ref[0]
        moment = beta_one * m_ref[0] + (1.0 - beta_one) * gradient.astype(jnp.float32)
        mo_ref[0] = moment
        left_high, left_low = split(l_ref[0])
        right_high, right_low = split(r_ref[0])
        moment_high, moment_low = split(moment)
        first = ((0,), (0,))
        grad_side = dot(left_high, gradient, first) + dot(left_low, gradient, first)
        moment_side = (
            dot(left_high, moment_high, first)
            + dot(left_high, moment_low, first)
            + dot(left_low, moment_high, first)
        )
        both_high, both_low = split(jnp.concatenate([grad_side, moment_side], axis=0))
        turned = dot(both_high, right_high) + dot(both_high, right_low) + dot(both_low, right_high)
        turned_gradient = turned[:width]
        turned_moment = turned[width:]
        second = beta_two * v_ref[0] + (1.0 - beta_two) * turned_gradient * turned_gradient
        vo_ref[0] = second
        bias_one = 1.0 - beta_one**STEP
        bias_two = 1.0 - beta_two**STEP
        scaled = turned_moment / bias_one / (jnp.sqrt(second / bias_two) + epsilon)
        scaled_high, scaled_low = split(scaled)
        rows = pl.ds(pl.multiple_of(core_ref[0] * half, half), half)
        part_high, part_low = split(l_ref[0, rows])
        back = (
            dot(part_high, scaled_high) + dot(part_high, scaled_low) + dot(part_low, scaled_high)
        )
        back_high, back_low = split(back)
        last = ((1,), (1,))
        update = (
            dot(back_high, right_high, last)
            + dot(back_high, right_low, last)
            + dot(back_low, right_high, last)
        )
        peak = jnp.maximum(jnp.max(jnp.abs(update), axis=0, keepdims=True), 1e-30)
        q_ref[0] = jnp.round(update * (LEVELS / peak)).astype(jnp.int32).astype(jnp.int16)
        w_ref[0] = peak * (1.0 / LEVELS)

    @pl.when(jnp.logical_not(live))
    def _():
        mo_ref[...] = jnp.zeros_like(mo_ref)
        vo_ref[...] = jnp.zeros_like(vo_ref)
        q_ref[...] = jnp.zeros_like(q_ref)
        w_ref[...] = jnp.zeros_like(w_ref)


def place_kernel(first, table_ref, q_ref, w_ref, d_ref):
    s = pl.program_id(0)
    half = q_ref.shape[1] // 2
    live = table_ref[first + pl.num_programs(0) + s] > 0

    @pl.when(live)
    def _():
        for c in range(2):
            rows = pl.ds(c * half, half)
            d_ref[0, rows] = q_ref[0, rows].astype(jnp.int32).astype(jnp.float32) * w_ref[c, 0]

    @pl.when(jnp.logical_not(live))
    def _():
        d_ref[...] = jnp.zeros_like(d_ref)


def body(
    gradients, first_moment, second_moment, left_basis, right_basis, shard_starts, block_owners
):
    devices = lax.axis_size("fsdp")
    me = lax.axis_index("fsdp")
    core = lax.axis_index("dp")
    slots = gradients.shape[1]
    owned = first_moment.shape[0]
    width = gradients.shape[3]
    half = width // lax.axis_size("dp")
    places = SIDES * slots

    vmem = pl.BlockSpec(memory_space=pltpu.VMEM)
    dma = pltpu.SemaphoreType.DMA
    smem = pl.BlockSpec(memory_space=pltpu.SMEM)
    gathered, table = pl.pallas_call(
        functools.partial(gather_kernel, devices, slots, owned),
        out_shape=[
            jax.ShapeDtypeStruct((places, width, width), jnp.bfloat16),
            jax.ShapeDtypeStruct((2 * (owned + slots),), jnp.int32),
        ],
        in_specs=[smem, smem, vmem],
        out_specs=[vmem, smem],
        scratch_shapes=[
            pltpu.VMEM((slots, half, width), jnp.bfloat16),
            pltpu.VMEM((slots, half, width), jnp.bfloat16),
            dma((slots,)),
            dma((slots,)),
            dma((2 * slots,)),
            dma((3 * slots,)),
            dma((7 * slots,)),
            dma((SIDES * slots,)),
            dma((SIDES * slots,)),
        ],
        compiler_params=pltpu.CompilerParams(collective_id=0, has_side_effects=True),
        name="gather",
    )(shard_starts, block_owners, gradients)

    def by_own(j, table, core):
        return (j, 0, 0)

    square = (1, width, width)
    moment_new, second_next, packed, scales = pl.pallas_call(
        step_kernel,
        grid_spec=pltpu.PrefetchScalarGridSpec(
            num_scalar_prefetch=2,
            grid=(owned,),
            in_specs=[
                pl.BlockSpec(square, lambda j, table, core: (table[j], 0, 0)),
                pl.BlockSpec(square, by_own),
                pl.BlockSpec(square, by_own),
                pl.BlockSpec(square, by_own),
                pl.BlockSpec(square, by_own),
            ],
            out_specs=[
                pl.BlockSpec(square, by_own),
                pl.BlockSpec(square, by_own),
                pl.BlockSpec((1, half, width), by_own),
                pl.BlockSpec((1, 1, width), by_own),
            ],
        ),
        out_shape=[
            jax.ShapeDtypeStruct(first_moment.shape, jnp.float32),
            jax.ShapeDtypeStruct(first_moment.shape, jnp.float32),
            jax.ShapeDtypeStruct((owned, half, width), jnp.int16),
            jax.ShapeDtypeStruct((owned, 1, width), jnp.float32),
        ],
        name="step",
    )(table, core[None].astype(jnp.int32),
      gathered, first_moment, second_moment, left_basis, right_basis)

    items = owned + 1
    returned, return_scales = pl.pallas_call(
        functools.partial(return_kernel, devices, owned),
        out_shape=[
            jax.ShapeDtypeStruct((SIDES * owned, width, width), jnp.int16),
            jax.ShapeDtypeStruct((2, SIDES * owned, 1, width), jnp.float32),
        ],
        in_specs=[vmem, vmem],
        out_specs=[vmem, vmem],
        scratch_shapes=[
            pltpu.VMEM((owned, half, width), jnp.int16),
            pltpu.VMEM((owned, 1, width), jnp.float32),
            dma((items,)),
            dma((2 * items,)),
            dma((3 * items,)),
            dma((7 * items,)),
            dma((SIDES * items,)),
            dma((SIDES * items,)),
        ],
        compiler_params=pltpu.CompilerParams(collective_id=1, has_side_effects=True),
        name="give_back",
    )(packed, scales)

    base = 2 * owned
    direction = pl.pallas_call(
        functools.partial(place_kernel, base),
        grid_spec=pltpu.PrefetchScalarGridSpec(
            num_scalar_prefetch=1,
            grid=(slots,),
            in_specs=[
                pl.BlockSpec(square, lambda s, table: (table[base + s], 0, 0)),
                pl.BlockSpec((2, 1, 1, width), lambda s, table: (0, table[base + s], 0, 0)),
            ],
            out_specs=pl.BlockSpec(square, lambda s, table: (s, 0, 0)),
        ),
        out_shape=jax.ShapeDtypeStruct((slots, width, width), jnp.float32),
        name="place",
    )(table, returned, return_scales)
    return (direction, moment_new, second_next)


def solution(mesh):
    in_specs = (
        P("dp", "fsdp", None, None),
        P("fsdp", None, None),
        P("fsdp", None, None),
        P("fsdp", None, None),
        P("fsdp", None, None),
        P(),
        P(),
    )
    out_specs = (P("fsdp", None, None), P("fsdp", None, None), P("fsdp", None, None))
    return jax.shard_map(body, mesh=mesh, in_specs=in_specs, out_specs=out_specs, check_vma=False)
```

```python
import functools

import jax
import jax.numpy as jnp
from jax import lax
from jax.experimental import pallas as pl
from jax.experimental.pallas import tpu as pltpu
from jax.sharding import PartitionSpec as P

REACH = 2
SIDES = 2 * REACH + 1
STEP = 10
LEVELS = 32767.0

beta_one = 0.9
beta_two = 0.95
epsilon = 1e-08

MESH = pl.DeviceIdType.MESH


DIRECT = ((1, 2), (-1, 2), (1, -2), (-1, -2))

ONWARD = (
    ({1: (2,), 2: (4,)}, {2: (4,), -2: (-1,)}, {-2: (-4,), 2: (1,)}, {-2: (-4,), -1: (-2,)}),
    (
        {2: (4, 1)},
        {-1: (-4,), 3: (2,), 2: (4,)},
        {-2: (-4,), 1: (4,), -3: (-2,)},
        {-2: (-1, -4)},
    ),
)

HOPS = (
    {1: 1, 2: 1, -2: 2, -1: 3},
    {-1: 1, 2: 1, 1: 2, -2: 2, 3: 2},
    {-2: 1, 1: 1, -1: 2, 2: 2, -3: 2},
    {-1: 1, -2: 1, 2: 2, 1: 3},
)


def guarded(condition, action):
    if condition is None:
        action()
    else:
        pl.when(condition)(action)


def greet(me, core, devices):
    barrier = pltpu.get_barrier_semaphore()
    x = jnp.where(me % 2 == 0, me + 1, me - 1)
    y = jnp.where(me % 4 < 2, me + 2, me - 2)
    pl.semaphore_signal(barrier, inc=1, device_id={"dp": 1 - core}, device_id_type=MESH)
    pl.semaphore_signal(barrier, inc=1, device_id={"fsdp": x}, device_id_type=MESH)
    pl.semaphore_signal(barrier, inc=1, device_id={"fsdp": y}, device_id_type=MESH)

    @pl.when(me >= 4)
    def _():
        pl.semaphore_signal(barrier, inc=1, device_id={"fsdp": me - 4}, device_id_type=MESH)

    @pl.when(me + 4 < devices)
    def _():
        pl.semaphore_signal(barrier, inc=1, device_id={"fsdp": me + 4}, device_id_type=MESH)

    return barrier


def met(barrier, me, devices):
    outer = jnp.where(me >= 4, 1, 0) + jnp.where(me + 4 < devices, 1, 0)
    pl.semaphore_wait(barrier, 3 + outer)


def relay(me, place, core, devices, items, own, ready, land, osend, fsend, recv, dsend, drecv):
    partner = {"dp": 1 - core}
    below, above = me >= 4, me + 4 < devices

    def reach(step):
        to = place + step
        return below if to < 0 else above if to > 3 else None

    def own_copy(way, i):
        hop = DIRECT[place][way]
        return pltpu.make_async_remote_copy(
            own(i), land(-hop, i, core), osend.at[way * items + i],
            recv.at[(3 - hop) * items + i], {"fsdp": me + hop}, MESH,
        )

    routes = [(off, hop) for off, hops in ONWARD[core][place].items() for hop in hops]

    def onward(off, hop, i):
        return pltpu.make_async_remote_copy(
            land(off, i, core), land(off - hop, i, core),
            fsend.at[routes.index((off, hop)) * items + i],
            recv.at[(off - hop + 3) * items + i], {"fsdp": me + hop}, MESH,
        )

    def arrival(off, i):
        at = recv.at[(off + 3) * items + i]
        ref = land(off, i, core)
        return pltpu.make_async_remote_copy(ref, ref, at, at, partner, MESH)

    def across(off, i, which):
        at = (off + REACH) * items + i
        source = own(i) if off == 0 else land(off, i, which)
        return pltpu.make_async_remote_copy(
            source, land(off, i, which), dsend.at[at], drecv.at[at], partner, MESH
        )

    offsets = [off for off in HOPS[place] if abs(off) <= REACH or off in ONWARD[core][place]]
    for i in range(items):
        ready(i)
        for way in range(2):
            own_copy(way, i).start()
        across(0, i, core).start()
    order = sorted((i + 2 * (HOPS[place][off] - 1), off, i) for off in offsets for i in range(items))
    for _, off, i in order:

        def arrive(off=off, i=i):
            arrival(off, i).wait_recv()
            for hop in ONWARD[core][place].get(off, ()):
                guarded(reach(hop), lambda hop=hop: onward(off, hop, i).start())
            if abs(off) <= REACH:
                across(off, i, core).start()

        guarded(reach(off), arrive)
    for i in range(items):
        for way in range(2):
            own_copy(way, i).wait_send()
        across(0, i, core).wait_send()
        across(0, i, 1 - core).wait_recv()
    for off in offsets:

        def finish(off=off):
            for i in range(items):
                for hop in ONWARD[core][place].get(off, ()):
                    guarded(reach(hop), lambda hop=hop, i=i: onward(off, hop, i).wait_send())
                if abs(off) <= REACH:
                    across(off, i, core).wait_send()
                    across(off, i, 1 - core).wait_recv()

        guarded(reach(off), finish)


def tables(me, devices, slots, owned, starts_ref, owners_ref, table_ref):
    blocks = owners_ref.shape[0]
    start = starts_ref[me]
    end = jnp.where(me + 1 < devices, starts_ref[jnp.minimum(me + 1, devices - 1)], blocks)
    held_owner = [owners_ref[jnp.minimum(start + s, blocks - 1)] for s in range(slots)]

    def count(b, carry):
        owner = owners_ref[b]
        below, mine, *ahead = carry
        return (
            below + (owner < me).astype(jnp.int32),
            mine + (owner == me).astype(jnp.int32),
            *[n + (owner < held_owner[s]).astype(jnp.int32) for s, n in enumerate(ahead)],
        )

    zero = jnp.int32(0)
    first, mine, *ahead = lax.fori_loop(0, blocks, count, (zero,) * (2 + slots))

    def seek(i, carry):
        begin = starts_ref[i]
        found = []
        for j in range(owned):
            holder, at = carry[j]
            passed = begin <= first + j
            found.append(
                (jnp.where(passed, i, holder), jnp.where(passed, begin, at))
            )
        return tuple(found)

    found = lax.fori_loop(0, devices, seek, ((zero, zero),) * owned)
    for j in range(owned):
        holder, at = found[j]
        live = j < mine
        table_ref[j] = jnp.where(live, (holder - me + REACH) * slots + first + j - at, 0)
        table_ref[owned + j] = live.astype(jnp.int32)
    for s in range(slots):
        live = start + s < end
        spot = (held_owner[s] - me + REACH) * owned + start + s - ahead[s]
        table_ref[2 * owned + s] = jnp.where(live, spot, 0)
        table_ref[2 * owned + slots + s] = live.astype(jnp.int32)


def each_place(me, core, run):
    for place in range(4):
        for side in range(2):

            @pl.when((me % 4 == place) & (core == side))
            def _():
                run(place, side)


def gather_kernel(
    devices, slots, owned, starts_ref, owners_ref, g_ref, out_ref, table_ref,
    part, transit, rs_send, rs_recv, osend, fsend, recv, dsend, drecv,
):
    me = lax.axis_index("fsdp")
    core = lax.axis_index("dp")
    half = g_ref.shape[2] // 2
    barrier = greet(me, core, devices)
    tables(me, devices, slots, owned, starts_ref, owners_ref, table_ref)
    met(barrier, me, devices)

    def run(place, side):
        mine, theirs = pl.ds(side * half, half), pl.ds((1 - side) * half, half)

        def reduce_copy(s):
            return pltpu.make_async_remote_copy(
                g_ref.at[0, s, theirs], part.at[s], rs_send.at[s], rs_recv.at[s],
                {"dp": 1 - side}, MESH,
            )

        def ready(s):
            reduce_copy(s).wait_recv()
            total = g_ref[0, s, mine].astype(jnp.float32) + part[s].astype(jnp.float32)
            out_ref[REACH * slots + s, mine] = total.astype(jnp.bfloat16)

        def land(off, s, which):
            if abs(off) > REACH:
                return transit.at[s]
            return out_ref.at[(off + REACH) * slots + s, pl.ds(which * half, half)]

        for s in range(slots):
            reduce_copy(s).start()
        relay(me, place, side, devices, slots, lambda s: land(0, s, side), ready, land,
              osend, fsend, recv, dsend, drecv)
        for s in range(slots):
            reduce_copy(s).wait_send()

    each_place(me, core, run)


def step_to(place, hop):
    return place if abs(hop) == 4 else place + hop


def upward(core, place, off):
    if off in DIRECT[place]:
        return off
    for hop in (1, -1, 2, -2, 4, -4):
        before = step_to(place, -hop)
        if 0 <= before < 4 and hop in ONWARD[core][before].get(off + hop, ()):
            return -hop
    raise ValueError(off)


def height(core, place, off):
    onward = ONWARD[core][place].get(off, ())
    return max((1 + height(core, step_to(place, hop), off - hop) for hop in onward), default=0)


def members(core, place, off, at):
    found = [at] if abs(off) <= REACH else []
    for hop in ONWARD[core][place].get(off, ()):
        found += members(core, step_to(place, hop), off - hop, at + hop)
    return found


def ports(core, place):
    routes = [(off, hop) for off, hops in ONWARD[core][place].items() for hop in hops]
    return [(0, hop) for hop in DIRECT[place]] + routes


def return_kernel(
    devices, slots, starts_ref, owners_ref, q_ref, w_ref, out_ref,
    arr_q, arr_w, pack_q, pack_w, send, recv, dsend, drecv,
):
    me = lax.axis_index("fsdp")
    core = lax.axis_index("dp")
    owned, half, _ = q_ref.shape
    blocks = owners_ref.shape[0]
    items = slots + 1
    barrier = greet(me, core, devices)
    first = lax.fori_loop(
        0, blocks, lambda b, n: n + (owners_ref[b] < me).astype(jnp.int32), jnp.int32(0)
    )
    picks = {}
    for off in range(-REACH, REACH + 1):
        holder = jnp.clip(me + off, 0, devices - 1)
        start = starts_ref[holder]
        after = starts_ref[jnp.minimum(holder + 1, devices - 1)]
        end = jnp.where(holder + 1 < devices, after, blocks)
        for s in range(slots):
            owner = owners_ref[jnp.minimum(start + s, blocks - 1)]
            at = jnp.clip(start + s - first, 0, owned - 1)
            picks[off, s] = (start + s < end, owner, at)
    met(barrier, me, devices)

    def run(place, side):
        mine, theirs = pl.ds(side * half, half), pl.ds((1 - side) * half, half)
        below, above = me >= 4, me + 4 < devices
        gates = ports(side, place)
        offsets = [off for off in HOPS[place] if abs(off) <= REACH or off in ONWARD[side][place]]

        def reach(step):
            to = place + step
            return below if to < 0 else above if to > 3 else None

        def inbox(port, i):
            return arr_w.at[port] if i == 0 else arr_q.at[port, i - 1]

        def send_copy(off, i):
            node = offsets.index(off)
            hop = upward(side, place, off)
            port = ports(side, step_to(place, hop)).index((off - hop, -hop))
            if abs(off) > REACH:
                source = inbox(gates.index((off, ONWARD[side][place][off][0])), i)
            else:
                source = pack_w.at[node] if i == 0 else pack_q.at[node, i - 1]
            return pltpu.make_async_remote_copy(
                source, inbox(port, i), send.at[node * items + i], recv.at[port * items + i],
                {"fsdp": me + hop}, MESH,
            )

        def arrival(port, i):
            at = recv.at[port * items + i]
            return pltpu.make_async_remote_copy(
                inbox(port, i), inbox(port, i), at, at, {"dp": 1 - side}, MESH
            )

        def chosen(off, s, own_ref, arrived):
            _, owner, at = picks[off, s]
            value = own_ref[at]
            onward = DIRECT[place] if off == 0 else ONWARD[side][place].get(off, ())
            if onward:
                came = arrived[gates.index((off, onward[-1])), s]
                if len(onward) == 2:
                    hop = onward[0]
                    group = members(side, step_to(place, hop), off - hop, hop)
                    inside = functools.reduce(jnp.logical_or, [owner == me + to for to in group])
                    came = lax.select(inside, arrived[gates.index((off, hop)), s], came)
                value = lax.select(owner == me, value, came)
            return value

        def collect(off, i):
            onward = DIRECT[place] if off == 0 else ONWARD[side][place].get(off, ())
            for hop in onward:
                port = gates.index((off, hop))
                guarded(reach(hop), lambda port=port: arrival(port, i).wait_recv())

        def pass_on(off, i):
            collect(off, i)
            node = offsets.index(off)
            if abs(off) <= REACH:
                if i == 0:
                    for s in range(slots):
                        pack_w[node, s] = chosen(off, s, w_ref, arr_w)
                else:
                    pack_q[node, i - 1] = chosen(off, i - 1, q_ref, arr_q)
            send_copy(off, i).start()

        def across(s, rows):
            return pltpu.make_async_remote_copy(
                out_ref.at[s, rows], out_ref.at[s, rows], dsend.at[s], drecv.at[s],
                {"dp": 1 - side}, MESH,
            )

        order = sorted(
            (i + 2 * height(side, place, off), off, i) for off in offsets for i in range(items)
        )
        for _, off, i in order:
            guarded(reach(off), lambda off=off, i=i: pass_on(off, i))
        collect(0, 0)
        for s in range(slots):
            collect(0, s + 1)
            value = chosen(0, s, q_ref, arr_q).astype(jnp.int32).astype(jnp.float32)
            value = value * chosen(0, s, w_ref, arr_w)
            out_ref[s, mine] = lax.select(picks[0, s][0], value, jnp.zeros_like(value))
            across(s, mine).start()
        for off in offsets:

            def finish(off=off):
                for i in range(items):
                    send_copy(off, i).wait_send()

            guarded(reach(off), finish)
        for s in range(slots):
            across(s, mine).wait_send()
            across(s, theirs).wait_recv()

    each_place(me, core, run)


def split(value):
    high = value.astype(jnp.bfloat16)
    low = (value - high.astype(jnp.float32)).astype(jnp.bfloat16)
    return high, low


def dot(a, b, dims=((1,), (0,))):
    return lax.dot_general(a, b, (dims, ((), ())), preferred_element_type=jnp.float32)


def step_kernel(table_ref, core_ref, g_ref, m_ref, v_ref, l_ref, r_ref,
                mo_ref, vo_ref, q_ref, w_ref):
    j = pl.program_id(0)
    half = q_ref.shape[1]
    width = g_ref.shape[2]
    live = table_ref[pl.num_programs(0) + j] > 0

    @pl.when(live)
    def _():
        gradient = g_ref[0]
        moment = beta_one * m_ref[0] + (1.0 - beta_one) * gradient.astype(jnp.float32)
        mo_ref[0] = moment
        left_high, left_low = split(l_ref[0])
        right_high, right_low = split(r_ref[0])
        moment_high, moment_low = split(moment)
        first = ((0,), (0,))
        grad_side = dot(left_high, gradient, first) + dot(left_low, gradient, first)
        moment_side = (
            dot(left_high, moment_high, first)
            + dot(left_high, moment_low, first)
            + dot(left_low, moment_high, first)
        )
        both_high, both_low = split(jnp.concatenate([grad_side, moment_side], axis=0))
        turned = dot(both_high, right_high) + dot(both_high, right_low) + dot(both_low, right_high)
        turned_gradient = turned[:width]
        turned_moment = turned[width:]
        second = beta_two * v_ref[0] + (1.0 - beta_two) * turned_gradient * turned_gradient
        vo_ref[0] = second
        bias_one = 1.0 - beta_one**STEP
        bias_two = 1.0 - beta_two**STEP
        scaled = turned_moment / bias_one / (jnp.sqrt(second / bias_two) + epsilon)
        scaled_high, scaled_low = split(scaled)
        rows = pl.ds(pl.multiple_of(core_ref[0] * half, half), half)
        part_high, part_low = split(l_ref[0, rows])
        back = (
            dot(part_high, scaled_high) + dot(part_high, scaled_low) + dot(part_low, scaled_high)
        )
        back_high, back_low = split(back)
        last = ((1,), (1,))
        update = (
            dot(back_high, right_high, last)
            + dot(back_high, right_low, last)
            + dot(back_low, right_high, last)
        )
        peak = jnp.maximum(jnp.max(jnp.abs(update), axis=0, keepdims=True), 1e-30)
        q_ref[0] = jnp.round(update * (LEVELS / peak)).astype(jnp.int32).astype(jnp.int16)
        w_ref[0] = peak * (1.0 / LEVELS)

    @pl.when(jnp.logical_not(live))
    def _():
        mo_ref[...] = jnp.zeros_like(mo_ref)
        vo_ref[...] = jnp.zeros_like(vo_ref)
        q_ref[...] = jnp.zeros_like(q_ref)
        w_ref[...] = jnp.zeros_like(w_ref)


def body(
    gradients, first_moment, second_moment, left_basis, right_basis, shard_starts, block_owners
):
    devices = lax.axis_size("fsdp")
    me = lax.axis_index("fsdp")
    core = lax.axis_index("dp")
    slots = gradients.shape[1]
    owned = first_moment.shape[0]
    width = gradients.shape[3]
    half = width // lax.axis_size("dp")
    places = SIDES * slots

    vmem = pl.BlockSpec(memory_space=pltpu.VMEM)
    dma = pltpu.SemaphoreType.DMA
    smem = pl.BlockSpec(memory_space=pltpu.SMEM)
    gathered, table = pl.pallas_call(
        functools.partial(gather_kernel, devices, slots, owned),
        out_shape=[
            jax.ShapeDtypeStruct((places, width, width), jnp.bfloat16),
            jax.ShapeDtypeStruct((2 * (owned + slots),), jnp.int32),
        ],
        in_specs=[smem, smem, vmem],
        out_specs=[vmem, smem],
        scratch_shapes=[
            pltpu.VMEM((slots, half, width), jnp.bfloat16),
            pltpu.VMEM((slots, half, width), jnp.bfloat16),
            dma((slots,)),
            dma((slots,)),
            dma((2 * slots,)),
            dma((3 * slots,)),
            dma((7 * slots,)),
            dma((SIDES * slots,)),
            dma((SIDES * slots,)),
        ],
        compiler_params=pltpu.CompilerParams(collective_id=0, has_side_effects=True),
        name="gather",
    )(shard_starts, block_owners, gradients)

    def by_own(j, table, core):
        return (j, 0, 0)

    square = (1, width, width)
    moment_new, second_next, packed, scales = pl.pallas_call(
        step_kernel,
        grid_spec=pltpu.PrefetchScalarGridSpec(
            num_scalar_prefetch=2,
            grid=(owned,),
            in_specs=[
                pl.BlockSpec(square, lambda j, table, core: (table[j], 0, 0)),
                pl.BlockSpec(square, by_own),
                pl.BlockSpec(square, by_own),
                pl.BlockSpec(square, by_own),
                pl.BlockSpec(square, by_own),
            ],
            out_specs=[
                pl.BlockSpec(square, by_own),
                pl.BlockSpec(square, by_own),
                pl.BlockSpec((1, half, width), by_own),
                pl.BlockSpec((1, 1, width), by_own),
            ],
        ),
        out_shape=[
            jax.ShapeDtypeStruct(first_moment.shape, jnp.float32),
            jax.ShapeDtypeStruct(first_moment.shape, jnp.float32),
            jax.ShapeDtypeStruct((owned, half, width), jnp.int16),
            jax.ShapeDtypeStruct((owned, 1, width), jnp.float32),
        ],
        name="step",
    )(table, core[None].astype(jnp.int32),
      gathered, first_moment, second_moment, left_basis, right_basis)

    items = slots + 1
    direction = pl.pallas_call(
        functools.partial(return_kernel, devices, slots),
        out_shape=jax.ShapeDtypeStruct((slots, width, width), jnp.float32),
        in_specs=[smem, smem, vmem, vmem],
        out_specs=vmem,
        scratch_shapes=[
            pltpu.VMEM((5, slots, half, width), jnp.int16),
            pltpu.VMEM((5, slots, 1, width), jnp.float32),
            pltpu.VMEM((5, slots, half, width), jnp.int16),
            pltpu.VMEM((5, slots, 1, width), jnp.float32),
            dma((5 * items,)),
            dma((5 * items,)),
            dma((slots,)),
            dma((slots,)),
        ],
        compiler_params=pltpu.CompilerParams(collective_id=1, has_side_effects=True),
        name="give_back",
    )(shard_starts, block_owners, packed, scales)
    return (direction, moment_new, second_next)


def solution(mesh):
    in_specs = (
        P("dp", "fsdp", None, None),
        P("fsdp", None, None),
        P("fsdp", None, None),
        P("fsdp", None, None),
        P("fsdp", None, None),
        P(),
        P(),
    )
    out_specs = (P("fsdp", None, None), P("fsdp", None, None), P("fsdp", None, None))
    return jax.shard_map(body, mesh=mesh, in_specs=in_specs, out_specs=out_specs, check_vma=False)
```

```python
import functools

import jax
import jax.numpy as jnp
from jax import lax
from jax.experimental import pallas as pl
from jax.experimental.pallas import tpu as pltpu
from jax.sharding import PartitionSpec as P

REACH = 2
SIDES = 2 * REACH + 1
STEP = 10
LEVELS = 32767.0

beta_one = 0.9
beta_two = 0.95
epsilon = 1e-08

MESH = pl.DeviceIdType.MESH


DIRECT = ((1, 2), (-1, 2), (1, -2), (-1, -2))

ONWARD = (
    ({1: (2,), 2: (4,)}, {2: (4,), -2: (-1,)}, {-2: (-4,), 2: (1,)}, {-2: (-4,), -1: (-2,)}),
    (
        {2: (4, 1)},
        {-1: (-4,), 3: (2,), 2: (4,)},
        {-2: (-4,), 1: (4,), -3: (-2,)},
        {-2: (-1, -4)},
    ),
)

HOPS = (
    {1: 1, 2: 1, -2: 2, -1: 3},
    {-1: 1, 2: 1, 1: 2, -2: 2, 3: 2},
    {-2: 1, 1: 1, -1: 2, 2: 2, -3: 2},
    {-1: 1, -2: 1, 2: 2, 1: 3},
)


def guarded(condition, action):
    if condition is None:
        action()
    else:
        pl.when(condition)(action)


def greet(me, core, devices):
    barrier = pltpu.get_barrier_semaphore()
    x = jnp.where(me % 2 == 0, me + 1, me - 1)
    y = jnp.where(me % 4 < 2, me + 2, me - 2)
    pl.semaphore_signal(barrier, inc=1, device_id={"dp": 1 - core}, device_id_type=MESH)
    pl.semaphore_signal(barrier, inc=1, device_id={"fsdp": x}, device_id_type=MESH)
    pl.semaphore_signal(barrier, inc=1, device_id={"fsdp": y}, device_id_type=MESH)

    @pl.when(me >= 4)
    def _():
        pl.semaphore_signal(barrier, inc=1, device_id={"fsdp": me - 4}, device_id_type=MESH)

    @pl.when(me + 4 < devices)
    def _():
        pl.semaphore_signal(barrier, inc=1, device_id={"fsdp": me + 4}, device_id_type=MESH)

    return barrier


def met(barrier, me, devices):
    outer = jnp.where(me >= 4, 1, 0) + jnp.where(me + 4 < devices, 1, 0)
    pl.semaphore_wait(barrier, 3 + outer)


def relay(me, place, core, devices, items, own, ready, land, osend, fsend, recv, dsend, drecv):
    partner = {"dp": 1 - core}
    below, above = me >= 4, me + 4 < devices

    def reach(step):
        to = place + step
        return below if to < 0 else above if to > 3 else None

    def own_copy(way, i):
        hop = DIRECT[place][way]
        return pltpu.make_async_remote_copy(
            own(i), land(-hop, i, core), osend.at[way * items + i],
            recv.at[(3 - hop) * items + i], {"fsdp": me + hop}, MESH,
        )

    routes = [(off, hop) for off, hops in ONWARD[core][place].items() for hop in hops]

    def onward(off, hop, i):
        return pltpu.make_async_remote_copy(
            land(off, i, core), land(off - hop, i, core),
            fsend.at[routes.index((off, hop)) * items + i],
            recv.at[(off - hop + 3) * items + i], {"fsdp": me + hop}, MESH,
        )

    def arrival(off, i):
        at = recv.at[(off + 3) * items + i]
        ref = land(off, i, core)
        return pltpu.make_async_remote_copy(ref, ref, at, at, partner, MESH)

    def across(off, i, which):
        at = (off + REACH) * items + i
        source = own(i) if off == 0 else land(off, i, which)
        return pltpu.make_async_remote_copy(
            source, land(off, i, which), dsend.at[at], drecv.at[at], partner, MESH
        )

    offsets = [off for off in HOPS[place] if abs(off) <= REACH or off in ONWARD[core][place]]
    for i in range(items):
        ready(i)
        for way in range(2):
            own_copy(way, i).start()
        across(0, i, core).start()
    order = sorted((i + 2 * (HOPS[place][off] - 1), off, i) for off in offsets for i in range(items))
    for _, off, i in order:

        def arrive(off=off, i=i):
            arrival(off, i).wait_recv()
            for hop in ONWARD[core][place].get(off, ()):
                guarded(reach(hop), lambda hop=hop: onward(off, hop, i).start())
            if abs(off) <= REACH:
                across(off, i, core).start()

        guarded(reach(off), arrive)
    for i in range(items):
        for way in range(2):
            own_copy(way, i).wait_send()
        across(0, i, core).wait_send()
        across(0, i, 1 - core).wait_recv()
    for off in offsets:

        def finish(off=off):
            for i in range(items):
                for hop in ONWARD[core][place].get(off, ()):
                    guarded(reach(hop), lambda hop=hop, i=i: onward(off, hop, i).wait_send())
                if abs(off) <= REACH:
                    across(off, i, core).wait_send()
                    across(off, i, 1 - core).wait_recv()

        guarded(reach(off), finish)


def tables(me, devices, slots, owned, starts_ref, owners_ref, table_ref):
    blocks = owners_ref.shape[0]
    start = starts_ref[me]
    end = jnp.where(me + 1 < devices, starts_ref[jnp.minimum(me + 1, devices - 1)], blocks)
    held_owner = [owners_ref[jnp.minimum(start + s, blocks - 1)] for s in range(slots)]

    def count(b, carry):
        owner = owners_ref[b]
        below, mine, *ahead = carry
        return (
            below + (owner < me).astype(jnp.int32),
            mine + (owner == me).astype(jnp.int32),
            *[n + (owner < held_owner[s]).astype(jnp.int32) for s, n in enumerate(ahead)],
        )

    zero = jnp.int32(0)
    first, mine, *ahead = lax.fori_loop(0, blocks, count, (zero,) * (2 + slots))

    def seek(i, carry):
        begin = starts_ref[i]
        found = []
        for j in range(owned):
            holder, at = carry[j]
            passed = begin <= first + j
            found.append(
                (jnp.where(passed, i, holder), jnp.where(passed, begin, at))
            )
        return tuple(found)

    found = lax.fori_loop(0, devices, seek, ((zero, zero),) * owned)
    for j in range(owned):
        holder, at = found[j]
        live = j < mine
        table_ref[j] = jnp.where(live, (holder - me + REACH) * slots + first + j - at, 0)
        table_ref[owned + j] = live.astype(jnp.int32)
    for s in range(slots):
        live = start + s < end
        spot = (held_owner[s] - me + REACH) * owned + start + s - ahead[s]
        table_ref[2 * owned + s] = jnp.where(live, spot, 0)
        table_ref[2 * owned + slots + s] = live.astype(jnp.int32)


def each_place(me, core, run):
    for place in range(4):
        for side in range(2):

            @pl.when((me % 4 == place) & (core == side))
            def _():
                run(place, side)


def gather_kernel(
    devices, slots, owned, starts_ref, owners_ref, g_ref, out_ref, table_ref,
    landed, part, transit, rs_send, rs_recv, osend, fsend, recv, dsend, drecv,
):
    me = lax.axis_index("fsdp")
    core = lax.axis_index("dp")
    half = g_ref.shape[2] // 2
    barrier = greet(me, core, devices)
    tables(me, devices, slots, owned, starts_ref, owners_ref, table_ref)
    met(barrier, me, devices)

    def run(place, side):
        mine, theirs = pl.ds(side * half, half), pl.ds((1 - side) * half, half)

        def reduce_copy(s):
            return pltpu.make_async_remote_copy(
                g_ref.at[0, s, theirs], part.at[s], rs_send.at[s], rs_recv.at[s],
                {"dp": 1 - side}, MESH,
            )

        def ready(s):
            reduce_copy(s).wait_recv()
            total = g_ref[0, s, mine].astype(jnp.float32) + part[s].astype(jnp.float32)
            landed[REACH * slots + s, mine] = total.astype(jnp.bfloat16)

        def land(off, s, which):
            if abs(off) > REACH:
                return transit.at[s]
            return landed.at[(off + REACH) * slots + s, pl.ds(which * half, half)]

        for s in range(slots):
            reduce_copy(s).start()
        relay(me, place, side, devices, slots, lambda s: land(0, s, side), ready, land,
              osend, fsend, recv, dsend, drecv)
        for s in range(slots):
            reduce_copy(s).wait_send()

    each_place(me, core, run)
    for j in range(owned):
        out_ref[j] = landed[jnp.clip(table_ref[j], 0, SIDES * slots - 1)]


def step_to(place, hop):
    return place if abs(hop) == 4 else place + hop


def upward(core, place, off):
    if off in DIRECT[place]:
        return off
    for hop in (1, -1, 2, -2, 4, -4):
        before = step_to(place, -hop)
        if 0 <= before < 4 and hop in ONWARD[core][before].get(off + hop, ()):
            return -hop
    raise ValueError(off)


def height(core, place, off):
    onward = ONWARD[core][place].get(off, ())
    return max((1 + height(core, step_to(place, hop), off - hop) for hop in onward), default=0)


def members(core, place, off, at):
    found = [at] if abs(off) <= REACH else []
    for hop in ONWARD[core][place].get(off, ()):
        found += members(core, step_to(place, hop), off - hop, at + hop)
    return found


def ports(core, place):
    routes = [(off, hop) for off, hops in ONWARD[core][place].items() for hop in hops]
    return [(0, hop) for hop in DIRECT[place]] + routes


def return_kernel(
    devices, slots, starts_ref, owners_ref, q_ref, w_ref, out_ref,
    arr_q, arr_w, pack_q, pack_w, send, recv, dsend, drecv,
):
    me = lax.axis_index("fsdp")
    core = lax.axis_index("dp")
    owned, half, _ = q_ref.shape
    blocks = owners_ref.shape[0]
    items = slots + 1
    barrier = greet(me, core, devices)
    first = lax.fori_loop(
        0, blocks, lambda b, n: n + (owners_ref[b] < me).astype(jnp.int32), jnp.int32(0)
    )
    picks = {}
    for off in range(-REACH, REACH + 1):
        holder = jnp.clip(me + off, 0, devices - 1)
        start = starts_ref[holder]
        after = starts_ref[jnp.minimum(holder + 1, devices - 1)]
        end = jnp.where(holder + 1 < devices, after, blocks)
        for s in range(slots):
            owner = owners_ref[jnp.minimum(start + s, blocks - 1)]
            at = jnp.clip(start + s - first, 0, owned - 1)
            picks[off, s] = (start + s < end, owner, at)
    met(barrier, me, devices)

    def run(place, side):
        mine, theirs = pl.ds(side * half, half), pl.ds((1 - side) * half, half)
        below, above = me >= 4, me + 4 < devices
        gates = ports(side, place)
        offsets = [off for off in HOPS[place] if abs(off) <= REACH or off in ONWARD[side][place]]

        def reach(step):
            to = place + step
            return below if to < 0 else above if to > 3 else None

        def inbox(port, i):
            return arr_w.at[port] if i == 0 else arr_q.at[port, i - 1]

        def send_copy(off, i):
            node = offsets.index(off)
            hop = upward(side, place, off)
            port = ports(side, step_to(place, hop)).index((off - hop, -hop))
            if abs(off) > REACH:
                source = inbox(gates.index((off, ONWARD[side][place][off][0])), i)
            else:
                source = pack_w.at[node] if i == 0 else pack_q.at[node, i - 1]
            return pltpu.make_async_remote_copy(
                source, inbox(port, i), send.at[node * items + i], recv.at[port * items + i],
                {"fsdp": me + hop}, MESH,
            )

        def arrival(port, i):
            at = recv.at[port * items + i]
            return pltpu.make_async_remote_copy(
                inbox(port, i), inbox(port, i), at, at, {"dp": 1 - side}, MESH
            )

        def chosen(off, s, own_ref, arrived):
            _, owner, at = picks[off, s]
            value = own_ref[at]
            onward = DIRECT[place] if off == 0 else ONWARD[side][place].get(off, ())
            if onward:
                came = arrived[gates.index((off, onward[-1])), s]
                if len(onward) == 2:
                    hop = onward[0]
                    group = members(side, step_to(place, hop), off - hop, hop)
                    inside = functools.reduce(jnp.logical_or, [owner == me + to for to in group])
                    came = lax.select(inside, arrived[gates.index((off, hop)), s], came)
                value = lax.select(owner == me, value, came)
            return value

        def collect(off, i):
            onward = DIRECT[place] if off == 0 else ONWARD[side][place].get(off, ())
            for hop in onward:
                port = gates.index((off, hop))
                guarded(reach(hop), lambda port=port: arrival(port, i).wait_recv())

        def pass_on(off, i):
            collect(off, i)
            node = offsets.index(off)
            if abs(off) <= REACH:
                if i == 0:
                    for s in range(slots):
                        pack_w[node, s] = chosen(off, s, w_ref, arr_w)
                else:
                    pack_q[node, i - 1] = chosen(off, i - 1, q_ref, arr_q)
            send_copy(off, i).start()

        def across(s, rows):
            return pltpu.make_async_remote_copy(
                out_ref.at[s, rows], out_ref.at[s, rows], dsend.at[s], drecv.at[s],
                {"dp": 1 - side}, MESH,
            )

        order = sorted(
            (i + 2 * height(side, place, off), off, i) for off in offsets for i in range(items)
        )
        for _, off, i in order:
            guarded(reach(off), lambda off=off, i=i: pass_on(off, i))
        collect(0, 0)
        for s in range(slots):
            collect(0, s + 1)
            value = chosen(0, s, q_ref, arr_q).astype(jnp.int32).astype(jnp.float32)
            value = value * chosen(0, s, w_ref, arr_w)
            out_ref[s, mine] = lax.select(picks[0, s][0], value, jnp.zeros_like(value))
            across(s, mine).start()
        for off in offsets:

            def finish(off=off):
                for i in range(items):
                    send_copy(off, i).wait_send()

            guarded(reach(off), finish)
        for s in range(slots):
            across(s, mine).wait_send()
            across(s, theirs).wait_recv()

    each_place(me, core, run)


def split(value):
    high = value.astype(jnp.bfloat16)
    low = (value - high.astype(jnp.float32)).astype(jnp.bfloat16)
    return high, low


def dot(a, b, dims=((1,), (0,))):
    return lax.dot_general(a, b, (dims, ((), ())), preferred_element_type=jnp.float32)


def step_kernel(table_ref, core_ref, g_ref, m_ref, v_ref, l_ref, r_ref,
                mo_ref, vo_ref, q_ref, w_ref):
    j = pl.program_id(0)
    half = q_ref.shape[1]
    width = g_ref.shape[2]
    live = table_ref[pl.num_programs(0) + j] > 0

    @pl.when(live)
    def _():
        gradient = g_ref[0]
        moment = beta_one * m_ref[0] + (1.0 - beta_one) * gradient.astype(jnp.float32)
        mo_ref[0] = moment
        turn_high, turn_low = split(l_ref[0].T)
        right_high, right_low = split(r_ref[0])
        moment_high, moment_low = split(moment)
        pair = jnp.concatenate([gradient, moment_high], axis=1)
        sides = dot(turn_high, pair) + dot(turn_low, pair)
        grad_side = sides[:, :width]
        moment_side = sides[:, width:] + dot(turn_high, moment_low)
        both_high, both_low = split(jnp.concatenate([grad_side, moment_side], axis=0))
        turned = dot(both_high, right_high) + dot(both_high, right_low) + dot(both_low, right_high)
        turned_gradient = turned[:width]
        turned_moment = turned[width:]
        second = beta_two * v_ref[0] + (1.0 - beta_two) * turned_gradient * turned_gradient
        vo_ref[0] = second
        bias_one = 1.0 - beta_one**STEP
        bias_two = 1.0 - beta_two**STEP
        scaled = turned_moment / bias_one / (jnp.sqrt(second / bias_two) + epsilon)
        scaled_high, scaled_low = split(scaled)
        rows = pl.ds(pl.multiple_of(core_ref[0] * half, half), half)
        part_high, part_low = split(l_ref[0, rows])
        back = (
            dot(part_high, scaled_high) + dot(part_high, scaled_low) + dot(part_low, scaled_high)
        )
        back_high, back_low = split(back)
        last = ((1,), (1,))
        update = (
            dot(back_high, right_high, last)
            + dot(back_high, right_low, last)
            + dot(back_low, right_high, last)
        )
        peak = jnp.maximum(jnp.max(jnp.abs(update), axis=0, keepdims=True), 1e-30)
        q_ref[0] = jnp.round(update * (LEVELS / peak)).astype(jnp.int32).astype(jnp.int16)
        w_ref[0] = peak * (1.0 / LEVELS)

    @pl.when(jnp.logical_not(live))
    def _():
        mo_ref[...] = jnp.zeros_like(mo_ref)
        vo_ref[...] = jnp.zeros_like(vo_ref)
        q_ref[...] = jnp.zeros_like(q_ref)
        w_ref[...] = jnp.zeros_like(w_ref)


def body(
    gradients, first_moment, second_moment, left_basis, right_basis, shard_starts, block_owners
):
    devices = lax.axis_size("fsdp")
    me = lax.axis_index("fsdp")
    core = lax.axis_index("dp")
    slots = gradients.shape[1]
    owned = first_moment.shape[0]
    width = gradients.shape[3]
    half = width // lax.axis_size("dp")
    places = SIDES * slots

    vmem = pl.BlockSpec(memory_space=pltpu.VMEM)
    dma = pltpu.SemaphoreType.DMA
    smem = pl.BlockSpec(memory_space=pltpu.SMEM)
    gathered, table = pl.pallas_call(
        functools.partial(gather_kernel, devices, slots, owned),
        out_shape=[
            jax.ShapeDtypeStruct((owned, width, width), jnp.bfloat16),
            jax.ShapeDtypeStruct((2 * (owned + slots),), jnp.int32),
        ],
        in_specs=[smem, smem, vmem],
        out_specs=[vmem, smem],
        scratch_shapes=[
            pltpu.VMEM((places, width, width), jnp.bfloat16),
            pltpu.VMEM((slots, half, width), jnp.bfloat16),
            pltpu.VMEM((slots, half, width), jnp.bfloat16),
            dma((slots,)),
            dma((slots,)),
            dma((2 * slots,)),
            dma((3 * slots,)),
            dma((7 * slots,)),
            dma((SIDES * slots,)),
            dma((SIDES * slots,)),
        ],
        compiler_params=pltpu.CompilerParams(collective_id=0, has_side_effects=True),
        name="gather",
    )(shard_starts, block_owners, gradients)

    def by_own(j, table, core):
        return (j, 0, 0)

    square = (1, width, width)
    moment_new, second_next, packed, scales = pl.pallas_call(
        step_kernel,
        grid_spec=pltpu.PrefetchScalarGridSpec(
            num_scalar_prefetch=2,
            grid=(owned,),
            in_specs=[
                pl.BlockSpec(square, by_own),
                pl.BlockSpec(square, by_own),
                pl.BlockSpec(square, by_own),
                pl.BlockSpec(square, by_own),
                pl.BlockSpec(square, by_own),
            ],
            out_specs=[
                pl.BlockSpec(square, by_own),
                pl.BlockSpec(square, by_own),
                pl.BlockSpec((1, half, width), by_own),
                pl.BlockSpec((1, 1, width), by_own),
            ],
        ),
        out_shape=[
            jax.ShapeDtypeStruct(first_moment.shape, jnp.float32),
            jax.ShapeDtypeStruct(first_moment.shape, jnp.float32),
            jax.ShapeDtypeStruct((owned, half, width), jnp.int16),
            jax.ShapeDtypeStruct((owned, 1, width), jnp.float32),
        ],
        name="step",
    )(table, core[None].astype(jnp.int32),
      gathered, first_moment, second_moment, left_basis, right_basis)

    items = slots + 1
    direction = pl.pallas_call(
        functools.partial(return_kernel, devices, slots),
        out_shape=jax.ShapeDtypeStruct((slots, width, width), jnp.float32),
        in_specs=[smem, smem, vmem, vmem],
        out_specs=vmem,
        scratch_shapes=[
            pltpu.VMEM((5, slots, half, width), jnp.int16),
            pltpu.VMEM((5, slots, 1, width), jnp.float32),
            pltpu.VMEM((5, slots, half, width), jnp.int16),
            pltpu.VMEM((5, slots, 1, width), jnp.float32),
            dma((5 * items,)),
            dma((5 * items,)),
            dma((slots,)),
            dma((slots,)),
        ],
        compiler_params=pltpu.CompilerParams(collective_id=1, has_side_effects=True),
        name="give_back",
    )(shard_starts, block_owners, packed, scales)
    return (direction, moment_new, second_next)


def solution(mesh):
    in_specs = (
        P("dp", "fsdp", None, None),
        P("fsdp", None, None),
        P("fsdp", None, None),
        P("fsdp", None, None),
        P("fsdp", None, None),
        P(),
        P(),
    )
    out_specs = (P("fsdp", None, None), P("fsdp", None, None), P("fsdp", None, None))
    return jax.shard_map(body, mesh=mesh, in_specs=in_specs, out_specs=out_specs, check_vma=False)
```
